32 devices in a mesh: bucket: 4 (over y, x), seq: 8 (over z, core).
Axes of the slice: x: 2, y: 2, z: 4, core: 2. Of those that a mesh axis runs over, the one named last changes fastest.
Arguments:
- queries: bfloat16 [4, 448, 1536], P('bucket', 'seq'), may hold values from -45 to 45, as said below
- keys: bfloat16 [4, 448, 1536], P('bucket', 'seq'), may hold values from -5 to 5
- values: bfloat16 [4, 448, 1536], P('bucket', 'seq'), may hold values from -6 to 6
- bucket_lens: int32 [4], P('bucket'), may hold values from 224 to 392
- gate: float32 [4, 3072], P('bucket'), may hold values from 0.5 to 2
- out_weight: bfloat16 [1536, 3072], P(None, 'bucket'), may hold values from -0.15625 to 0.15625
Outputs:
- gated_out: bfloat16 [4, 448, 3072], P('bucket', 'seq')
The draws below stay inside these ranges and needn't reach their ends.
Inputs may be any that keep to these rules, and one draw needn't show every extreme that they name: queries of a few tokens in a bucket may be strong multiples of some keys.
All inputs are finite; a program needn't handle non-finite values.
Results may differ from the reference program's by a relative error of at most 0.013.
Values may be sent and summed in bfloat16 or wider, within the bound.
No kernel may reach another device: no remote copies, remote signals or barrier semaphores. Data moves between devices by JAX's collectives and lax.ppermute only.
A program may use at most 192 MiB of HBM per device.

```python
import jax
import jax.numpy as jnp
from jax import lax

D = 3072
HEADS = 12
HEAD_DIM = 128
TOK_DEV = 56
BUCKETS = 4
TOKENS = 448


def query_key_pair(key):
    base = jax.random.fold_in(key, 7)
    key_q, key_k = jax.random.split(base, 2)
    shape = (BUCKETS, TOKENS, HEADS * HEAD_DIM)
    queries = jnp.clip(1.6 * jax.random.normal(key_q, shape, jnp.float32), -5.0, 5.0)
    keys = jnp.clip(1.6 * jax.random.normal(key_k, shape, jnp.float32), -5.0, 5.0)
    return (queries, keys)


def draw_queries(key, part):
    return query_key_pair(key)[0].astype(jnp.bfloat16)


def draw_keys(key, part):
    return query_key_pair(key)[1].astype(jnp.bfloat16)


def with_ends(entries, stream_key, smallest, largest):
    longest = entries.shape.index(max(entries.shape))
    spots = []
    for shift in (0, 1):
        where = [jax.random.randint(jax.random.fold_in(stream_key, axis), (), 0, length) for axis, length in enumerate(entries.shape)]
        where[longest] = (where[longest] + shift) % entries.shape[longest]
        spots.append(tuple(where))
    return entries.at[spots[0]].set(smallest).at[spots[1]].set(largest)


def shard_levels(key, shape, pieces, low, high):
    loudness, own = 1.0, jax.random.fold_in(key, 6)
    for dim, blocks in pieces:
        steps = jnp.exp(jax.random.uniform(jax.random.fold_in(own, dim), (blocks,), jnp.float32, low / len(pieces), high / len(pieces)))
        loudness = loudness * jnp.repeat(steps, shape[dim] // blocks).reshape([-1 if axis == dim else 1 for axis in range(len(shape))])
    return loudness


def gaussian(own_key, dims, spread, limit, pieces=(), kind=jnp.bfloat16):
    array = jax.random.normal(own_key, dims, jnp.float32) * spread
    if len(pieces) > 0:
        array = shard_levels(own_key, dims, pieces, -0.22, 0.18) * array
    return jnp.clip(array, min=-limit, max=limit).astype(kind)


def setup_inputs(seed: int = 0) -> dict:
    streams_of = jax.random.split(jax.random.key(seed), 7)
    queries = draw_queries(jax.random.fold_in(streams_of[6], 71), 0)
    keys = draw_keys(jax.random.fold_in(streams_of[6], 71), 0)
    values = gaussian(streams_of[2], (BUCKETS, TOKENS, HEADS * HEAD_DIM), 1.0, 6.0, ((0, 4), (1, 8)))
    bucket_lens = with_ends(jax.random.randint(streams_of[3], (BUCKETS,), TOKENS // 2, TOKENS - TOK_DEV + 1), jax.random.fold_in(streams_of[3], 1), TOKENS // 2, TOKENS - TOK_DEV).astype(jnp.int32)
    gate = jnp.clip(0.5 + 1.5 * jax.random.uniform(streams_of[4], (BUCKETS, D), jnp.float32) ** shard_levels(streams_of[4], (BUCKETS, D), ((0, 4),), -0.2, 0.2), 0.5, 2.0)
    out_weight = gaussian(streams_of[5], (HEADS * HEAD_DIM, D), (HEADS * HEAD_DIM) ** -0.5, 0.15625, ((1, 4),))
    return dict(queries=queries, keys=keys, values=values, bucket_lens=bucket_lens, gate=gate, out_weight=out_weight)


NEG_FILL = -1.0e30


def block_stats(queries, keys, values, usable):
    scores = jnp.einsum("qhe,nkhe->nhqk", queries, keys) * (HEAD_DIM ** -0.5)
    keep_mask = usable[:, None, None, :]
    scores = jnp.where(keep_mask, scores, NEG_FILL)
    maxima = jnp.max(scores, axis=3)
    weights = jnp.where(keep_mask, jnp.exp(scores - maxima[..., None]), 0.0)
    totals = jnp.sum(weights, axis=3)
    rounded = lax.optimization_barrier(weights.astype(jnp.bfloat16)).astype(jnp.float32)
    weighted = jnp.einsum("nhqk,nkhe->nqhe", rounded, values)
    divisor = jnp.transpose(jnp.maximum(totals, 1.0), (0, 2, 1))
    partial_value = (weighted / divisor[..., None]).astype(jnp.bfloat16)
    return partial_value, jnp.transpose(maxima, (0, 2, 1)), jnp.transpose(totals, (0, 2, 1))


def combine(partial_value, maxima, totals):
    row_max = jnp.max(maxima, axis=0)
    factors = totals * jnp.exp(maxima - row_max[None])
    partial_wide = lax.optimization_barrier(partial_value).astype(jnp.float32)
    summed = jnp.einsum("nqh,nqhe->qhe", factors, partial_wide)
    attended = summed / jnp.sum(factors, axis=0)[..., None]
    return attended.reshape(attended.shape[0], -1).astype(jnp.bfloat16)


def reference(queries, keys, values, bucket_lens, gate, out_weight):
    count = queries.shape[1]
    block_count = count // TOK_DEV
    positions = jnp.arange(count, dtype=jnp.int32)
    results = []
    for bucket in range(queries.shape[0]):
        length = bucket_lens[bucket]
        key_blocks = keys[bucket].astype(jnp.float32).reshape(block_count, TOK_DEV, HEADS, HEAD_DIM)
        value_blocks = values[bucket].astype(jnp.float32).reshape(block_count, TOK_DEV, HEADS, HEAD_DIM)
        usable = (positions < length).reshape(block_count, TOK_DEV)
        query_blocks = queries[bucket].reshape(block_count, TOK_DEV, HEADS, HEAD_DIM)

        def one_block(query_block):
            partial_value, maxima, totals = block_stats(query_block.astype(jnp.float32), key_blocks, value_blocks, usable)
            return combine(partial_value, maxima, totals)

        attended = lax.map(one_block, query_blocks).reshape(count, HEADS * HEAD_DIM)
        projected = jnp.dot(attended, out_weight, preferred_element_type=jnp.float32) * gate[bucket][None, :]
        projected = jnp.where((positions < length)[:, None], projected, 0.0)
        results.append(projected.astype(jnp.bfloat16))
    return jnp.stack(results)
```

```python
import jax
import jax.numpy as jnp
from jax import lax
from jax.sharding import PartitionSpec as P

HEADS = 12
HEAD_DIM = 128
NEG_FILL = -1e30
ROW_LIMIT = 512


def head_windows(parts):
    share = HEADS * HEAD_DIM // parts
    first = [(share * d) // HEAD_DIM for d in range(parts)]
    last = [-(-share * (d + 1) // HEAD_DIM) for d in range(parts)]
    slots = max(b - a for a, b in zip(first, last))
    return [min(a, HEADS - slots) for a in first], slots


def attend(query, key, value, usable):
    scores = lax.dot_general(
        query, key, (((1,), (1,)), ((), ())), preferred_element_type=jnp.float32
    ) * HEAD_DIM ** (-0.5)
    scores = jnp.where(usable, scores, NEG_FILL)
    weights = jnp.exp(scores - jnp.max(scores, axis=1, keepdims=True))
    total = jnp.sum(weights, axis=1, keepdims=True)
    out = jnp.dot(weights.astype(jnp.bfloat16), value, preferred_element_type=jnp.float32)
    return (out / total).astype(jnp.bfloat16)


def attend_rows(query, key, value, usable):
    rows = query.shape[0]
    if rows <= ROW_LIMIT:
        return attend(query, key, value, usable)
    steps = next(n for n in range(1, rows + 1) if rows % n == 0 and rows // n <= ROW_LIMIT)
    blocks = query.reshape(steps, rows // steps, query.shape[1])
    return lax.map(lambda block: attend(block, key, value, usable), blocks).reshape(query.shape)


def make_shards(parts):
    first, slots = head_windows(parts)
    wide = slots * HEAD_DIM

    def shards(queries, keys, values, bucket_lens, gate, out_weight):
        rows_here = queries.shape[1]
        length = bucket_lens[0]
        position = lax.axis_index("seq") * rows_here + lax.iota(jnp.int32, rows_here)
        pieces = []
        for start in first:
            cut = slice(start * HEAD_DIM, start * HEAD_DIM + wide)
            pieces.append(
                jnp.concatenate([queries[0][:, cut], keys[0][:, cut], values[0][:, cut]], axis=1)
            )
        mine = lax.all_to_all(jnp.stack(pieces), "seq", split_axis=0, concat_axis=0, tiled=True)
        count_all = parts * rows_here
        mine = mine.reshape(count_all, 3 * wide)
        usable = (lax.iota(jnp.int32, count_all) < length)[None, :]
        outs = []
        for slot in range(slots):
            q, k, v = (
                mine[:, which * wide + slot * HEAD_DIM : which * wide + (slot + 1) * HEAD_DIM]
                for which in range(3)
            )
            outs.append(attend_rows(q, k, v, usable))
        outs = jnp.concatenate(outs, axis=1).reshape(parts, rows_here, wide)
        back = lax.all_to_all(outs, "seq", split_axis=0, concat_axis=0, tiled=True)
        columns = []
        for head in range(HEADS):
            source = next(d for d in range(parts) if first[d] <= head < first[d] + slots)
            slot = head - first[source]
            columns.append(back[source][:, slot * HEAD_DIM : (slot + 1) * HEAD_DIM])
        attended = jnp.concatenate(columns, axis=1)
        everyone = lax.all_gather(attended, "bucket", axis=0, tiled=True)
        projected = jnp.dot(everyone, out_weight, preferred_element_type=jnp.float32)
        projected = projected.astype(jnp.bfloat16).reshape(-1, rows_here, out_weight.shape[1])
        gathered = lax.all_to_all(projected, "bucket", split_axis=0, concat_axis=0, tiled=True)
        wide_rows = jnp.concatenate([gathered[c] for c in range(gathered.shape[0])], axis=1)
        result = wide_rows.astype(jnp.float32) * gate[0][None, :]
        return jnp.where((position < length)[:, None], result, 0.0).astype(jnp.bfloat16)[None]

    return shards


def solution(mesh):
    placed = (
        P("bucket", "seq", None),
        P("bucket", "seq", None),
        P("bucket", "seq", None),
        P("bucket"),
        P("bucket", None),
        P(None, "bucket"),
    )
    return jax.shard_map(
        make_shards(mesh.shape["seq"]),
        mesh=mesh, in_specs=placed, out_specs=P("bucket", "seq", None), check_vma=False,
    )
```

```python
import math

import jax
import jax.numpy as jnp
from jax import lax
from jax.experimental import pallas as pl
from jax.experimental.pallas import tpu as pltpu
from jax.sharding import PartitionSpec as P

HEADS = 12
HEAD_DIM = 128
NEG_FILL = -1e30

VMEM = pl.BlockSpec(memory_space=pltpu.VMEM)
SMEM = pl.BlockSpec(memory_space=pltpu.SMEM)


def cut_pieces(row, queries, keys, values, outer):
    rows, width = queries.shape
    share = width // outer

    def body(row_ref, q_ref, k_ref, v_ref, *outs):
        for k in range(outer):
            cut = pl.ds(pl.multiple_of((row_ref[0] ^ k) * share, HEAD_DIM), share)
            outs[k][:, :share] = k_ref[:, cut]
            outs[k][:, share:] = v_ref[:, cut]
            outs[outer + k][...] = q_ref[:, cut]

    shapes = [jax.ShapeDtypeStruct((rows, 2 * share), queries.dtype)] * outer
    shapes += [jax.ShapeDtypeStruct((rows, share), queries.dtype)] * outer
    out = pl.pallas_call(
        body, out_shape=shapes, in_specs=[SMEM, VMEM, VMEM, VMEM], out_specs=[VMEM] * (2 * outer),
        name="cut_pieces",
    )(row, queries, keys, values)
    return out[:outer], out[outer:]


def attend_pieces(usable, queries, pairs):
    rows_here, share = queries[0].shape
    outer = len(queries)
    key_rows = [p.shape[0] for p in pairs]

    def body(usable_ref, *refs):
        q_refs, pair_refs = refs[:outer], refs[outer : outer + len(pairs)]
        outs = refs[outer + len(pairs) :]
        keep = usable_ref[...] > 0
        for head in range(share // HEAD_DIM):
            cut = slice(head * HEAD_DIM, (head + 1) * HEAD_DIM)
            vcut = slice(share + head * HEAD_DIM, share + (head + 1) * HEAD_DIM)
            query = jnp.concatenate([r[:, cut] for r in q_refs], axis=0)
            key = jnp.concatenate([r[:, cut] for r in pair_refs], axis=0)
            value = jnp.concatenate([r[:, vcut] for r in pair_refs], axis=0)
            scores = lax.dot_general(
                query, key, (((1,), (1,)), ((), ())), preferred_element_type=jnp.float32
            ) * HEAD_DIM ** (-0.5)
            scores = jnp.where(keep, scores, NEG_FILL)
            weights = jnp.exp(scores - jnp.max(scores, axis=1, keepdims=True))
            total = jnp.sum(weights, axis=1, keepdims=True)
            out = jnp.dot(weights.astype(jnp.bfloat16), value, preferred_element_type=jnp.float32)
            out = (out / total).astype(jnp.bfloat16)
            for k in range(outer):
                outs[k][:, cut] = out[k * rows_here : (k + 1) * rows_here]

    return pl.pallas_call(
        body, out_shape=[jax.ShapeDtypeStruct((rows_here, share), jnp.bfloat16)] * outer,
        in_specs=[VMEM] * (1 + outer + len(pairs)), out_specs=[VMEM] * outer,
        name="attend_pieces",
    )(usable, *queries, *pairs)


def make_shards(parts):
    outer = math.gcd(4, parts // 2)
    inner = parts // outer
    same_outer = [[g * inner + i for i in range(inner)] for g in range(outer)]

    def send(piece, k):
        if k == 0:
            return piece
        return lax.ppermute(piece, "seq", [(s, s ^ (k * inner)) for s in range(parts)])

    def shards(queries, keys, values, bucket_lens, gate, out_weight):
        rows_here, width = queries.shape[1:]
        share = width // outer
        length = bucket_lens[0]
        here = lax.axis_index("seq")
        row, own = here // inner, here % inner
        position = here * rows_here + lax.iota(jnp.int32, rows_here)
        pairs, query = cut_pieces(row[None], queries[0], keys[0], values[0], outer)
        pairs = [send(p, k) for k, p in enumerate(pairs)]
        query = [send(p, k) for k, p in enumerate(query)]
        groups = row ^ lax.iota(jnp.int32, outer)
        if inner == 2:
            other = lax.ppermute(
                jnp.concatenate(pairs, axis=0), "seq", [(s, s ^ 1) for s in range(parts)]
            )
            pairs = pairs + [other]
            members = jnp.stack([own, 1 - own])
        else:
            pairs = [
                lax.all_gather(
                    jnp.concatenate(pairs, axis=0), "seq", axis=0, tiled=True,
                    axis_index_groups=same_outer,
                )
            ]
            members = lax.iota(jnp.int32, inner)
        places = (
            (groups[None, :, None] * inner + members[:, None, None]) * rows_here
            + lax.iota(jnp.int32, rows_here)[None, None, :]
        )
        usable = (places < length).astype(jnp.int32).reshape(1, -1)
        outs = attend_pieces(usable, query, pairs)
        back = [send(p, k) for k, p in enumerate(outs)]
        weight = jnp.concatenate(
            [lax.dynamic_slice_in_dim(out_weight, (row ^ k) * share, share, 0) for k in range(outer)], axis=0
        )
        attended = jnp.concatenate(back, axis=1)
        everyone = lax.all_gather(attended, "bucket", axis=0, tiled=True)
        projected = jnp.dot(everyone, weight, preferred_element_type=jnp.float32)
        projected = projected.astype(jnp.bfloat16).reshape(-1, rows_here, out_weight.shape[1])
        gathered = lax.all_to_all(projected, "bucket", split_axis=0, concat_axis=0, tiled=True)
        wide_rows = jnp.concatenate([gathered[c] for c in range(gathered.shape[0])], axis=1)
        result = wide_rows.astype(jnp.float32) * gate[0][None, :]
        return jnp.where((position < length)[:, None], result, 0.0).astype(jnp.bfloat16)[None]

    return shards


def solution(mesh):
    placed = (
        P("bucket", "seq", None),
        P("bucket", "seq", None),
        P("bucket", "seq", None),
        P("bucket"),
        P("bucket", None),
        P(None, "bucket"),
    )
    return jax.shard_map(
        make_shards(mesh.shape["seq"]),
        mesh=mesh, in_specs=placed, out_specs=P("bucket", "seq", None), check_vma=False,
    )
```

```python
import math

import jax
import jax.numpy as jnp
from jax import lax
from jax.experimental import pallas as pl
from jax.experimental.pallas import tpu as pltpu
from jax.sharding import PartitionSpec as P


HEAD_DIM = 128
NEG_FILL = -1e30

VMEM = pl.BlockSpec(memory_space=pltpu.VMEM)
SMEM = pl.BlockSpec(memory_space=pltpu.SMEM)


def cut_pieces(row, queries, keys, values, outer):
    rows, width = queries.shape
    share = width // outer

    def body(row_ref, q_ref, k_ref, v_ref, *outs):
        for k in range(outer):
            cut = pl.ds(pl.multiple_of((row_ref[0] ^ k) * share, HEAD_DIM), share)
            outs[k][:, :share] = k_ref[:, cut]
            outs[k][:, share:] = v_ref[:, cut]
            outs[outer + k][...] = q_ref[:, cut]

    shapes = [jax.ShapeDtypeStruct((rows, 2 * share), queries.dtype)] * outer
    shapes += [jax.ShapeDtypeStruct((rows, share), queries.dtype)] * outer
    out = pl.pallas_call(
        body, out_shape=shapes, in_specs=[SMEM, VMEM, VMEM, VMEM], out_specs=[VMEM] * (2 * outer),
        name="cut_pieces",
    )(row, queries, keys, values)
    return out[:outer], out[outer:]


def attend_pieces(usable, queries, pairs):
    rows_here, share = queries[0].shape
    outer = len(queries)

    def body(usable_ref, *refs):
        q_refs, pair_refs = refs[:outer], refs[outer : outer + len(pairs)]
        outs = refs[outer + len(pairs) :]
        keep = usable_ref[...] > 0
        scores, values = [], []
        for head in range(share // HEAD_DIM):
            cut = slice(head * HEAD_DIM, (head + 1) * HEAD_DIM)
            vcut = slice(share + head * HEAD_DIM, share + (head + 1) * HEAD_DIM)
            query = jnp.concatenate([r[:, cut] for r in q_refs], axis=0)
            key = jnp.concatenate([r[:, cut] for r in pair_refs], axis=0)
            values.append(jnp.concatenate([r[:, vcut] for r in pair_refs], axis=0))
            score = lax.dot_general(
                query, key, (((1,), (1,)), ((), ())), preferred_element_type=jnp.float32
            ) * HEAD_DIM ** (-0.5)
            scores.append(jnp.where(keep, score, NEG_FILL))
        weights = [jnp.exp(s - jnp.max(s, axis=1, keepdims=True)) for s in scores]
        results = []
        for weight, value in zip(weights, values):
            total = jnp.sum(weight, axis=1, keepdims=True)
            out = jnp.dot(weight.astype(jnp.bfloat16), value, preferred_element_type=jnp.float32)
            results.append((out * (1.0 / total)).astype(jnp.bfloat16))
        for head, out in enumerate(results):
            for k in range(outer):
                cut = slice(head * HEAD_DIM, (head + 1) * HEAD_DIM)
                outs[k][:, cut] = out[k * rows_here : (k + 1) * rows_here]

    return pl.pallas_call(
        body, out_shape=[jax.ShapeDtypeStruct((rows_here, share), jnp.bfloat16)] * outer,
        in_specs=[VMEM] * (1 + outer + len(pairs)), out_specs=[VMEM] * outer,
        name="attend_pieces",
    )(usable, *queries, *pairs)


def make_shards(parts):
    outer = math.gcd(4, parts // 2)
    inner = parts // outer
    same_outer = [[g * inner + i for i in range(inner)] for g in range(outer)]

    def send(piece, k):
        if k == 0:
            return piece
        return lax.ppermute(piece, "seq", [(s, s ^ (k * inner)) for s in range(parts)])

    def shards(queries, keys, values, bucket_lens, gate, out_weight):
        rows_here, width = queries.shape[1:]
        share = width // outer
        length = bucket_lens[0]
        here = lax.axis_index("seq")
        row, own = here // inner, here % inner
        position = here * rows_here + lax.iota(jnp.int32, rows_here)
        pairs, query = cut_pieces(row[None], queries[0], keys[0], values[0], outer)
        pairs = [send(p, k) for k, p in enumerate(pairs)]
        query = [send(p, k) for k, p in enumerate(query)]
        groups = row ^ lax.iota(jnp.int32, outer)
        if inner == 2:
            pairs = pairs + [
                lax.ppermute(p, "seq", [(s, s ^ 1) for s in range(parts)]) for p in pairs
            ]
            members = jnp.stack([own, 1 - own])
        else:
            pairs = [
                lax.all_gather(
                    jnp.concatenate(pairs, axis=0), "seq", axis=0, tiled=True,
                    axis_index_groups=same_outer,
                )
            ]
            members = lax.iota(jnp.int32, inner)
        places = (
            (groups[None, :, None] * inner + members[:, None, None]) * rows_here
            + lax.iota(jnp.int32, rows_here)[None, None, :]
        )
        usable = (places < length).astype(jnp.int32).reshape(1, -1)
        outs = attend_pieces(usable, query, pairs)
        back = [send(p, k) for k, p in enumerate(outs)]
        weight = jnp.concatenate(
            [lax.dynamic_slice_in_dim(out_weight, (row ^ k) * share, share, 0) for k in range(outer)], axis=0
        )
        attended = jnp.concatenate(back, axis=1)
        everyone = lax.all_gather(attended, "bucket", axis=0, tiled=True)
        projected = jnp.dot(everyone, weight, preferred_element_type=jnp.float32)
        projected = projected.astype(jnp.bfloat16).reshape(-1, rows_here, out_weight.shape[1])
        gathered = lax.all_to_all(projected, "bucket", split_axis=0, concat_axis=0, tiled=True)
        wide_rows = jnp.concatenate([gathered[c] for c in range(gathered.shape[0])], axis=1)
        result = wide_rows.astype(jnp.float32) * gate[0][None, :]
        return jnp.where((position < length)[:, None], result, 0.0).astype(jnp.bfloat16)[None]

    return shards


def solution(mesh):
    placed = (
        P("bucket", "seq", None),
        P("bucket", "seq", None),
        P("bucket", "seq", None),
        P("bucket"),
        P("bucket", None),
        P(None, "bucket"),
    )
    return jax.shard_map(
        make_shards(mesh.shape["seq"]),
        mesh=mesh, in_specs=placed, out_specs=P("bucket", "seq", None), check_vma=False,
    )
```

```python
import math

import jax
import jax.numpy as jnp
from jax import lax
from jax.experimental import pallas as pl
from jax.experimental.pallas import tpu as pltpu
from jax.sharding import PartitionSpec as P


HEAD_DIM = 128
NEG_FILL = -1e30

VMEM = pl.BlockSpec(memory_space=pltpu.VMEM)
SMEM = pl.BlockSpec(memory_space=pltpu.SMEM)


def cut_pieces(row, arrays, outer):
    rows, width = arrays[0].shape
    share = width // outer

    def body(row_ref, *refs):
        for k in range(outer):
            cut = pl.ds(pl.multiple_of((row_ref[0] ^ k) * share, HEAD_DIM), share)
            for which in range(len(arrays)):
                place = slice(which * share, (which + 1) * share)
                refs[len(arrays) + k][:, place] = refs[which][:, cut]

    shape = jax.ShapeDtypeStruct((rows, len(arrays) * share), arrays[0].dtype)
    return pl.pallas_call(
        body, out_shape=[shape] * outer, in_specs=[SMEM] + [VMEM] * len(arrays),
        out_specs=[VMEM] * outer, name="cut_pieces",
    )(row, *arrays)


def attend_pieces(usable, queries, pairs):
    rows_here, share = queries[0].shape
    outer = len(queries)

    def body(usable_ref, *refs):
        q_refs, pair_refs = refs[:outer], refs[outer : outer + len(pairs)]
        outs = refs[outer + len(pairs) :]
        keep = usable_ref[...] > 0
        scores, values = [], []
        for head in range(share // HEAD_DIM):
            cut = slice(head * HEAD_DIM, (head + 1) * HEAD_DIM)
            vcut = slice(share + head * HEAD_DIM, share + (head + 1) * HEAD_DIM)
            query = jnp.concatenate([r[:, cut] for r in q_refs], axis=0)
            key = jnp.concatenate([r[:, cut] for r in pair_refs], axis=0)
            values.append(jnp.concatenate([r[:, vcut] for r in pair_refs], axis=0))
            score = lax.dot_general(
                query, key, (((1,), (1,)), ((), ())), preferred_element_type=jnp.float32
            ) * HEAD_DIM ** (-0.5)
            scores.append(jnp.where(keep, score, NEG_FILL))
        weights = [jnp.exp(s - jnp.max(s, axis=1, keepdims=True)) for s in scores]
        results = []
        for weight, value in zip(weights, values):
            total = jnp.sum(weight, axis=1, keepdims=True)
            out = jnp.dot(weight.astype(jnp.bfloat16), value, preferred_element_type=jnp.float32)
            results.append((out * (1.0 / total)).astype(jnp.bfloat16))
        for head, out in enumerate(results):
            for k in range(outer):
                cut = slice(head * HEAD_DIM, (head + 1) * HEAD_DIM)
                outs[k][:, cut] = out[k * rows_here : (k + 1) * rows_here]

    return pl.pallas_call(
        body, out_shape=[jax.ShapeDtypeStruct((rows_here, share), jnp.bfloat16)] * outer,
        in_specs=[VMEM] * (1 + outer + len(pairs)), out_specs=[VMEM] * outer,
        name="attend_pieces",
    )(usable, *queries, *pairs)


def make_shards(parts):
    outer = math.gcd(4, parts // 2)
    inner = parts // outer
    same_outer = [[g * inner + i for i in range(inner)] for g in range(outer)]

    def send(piece, k):
        if k == 0:
            return piece
        return lax.ppermute(piece, "seq", [(s, s ^ (k * inner)) for s in range(parts)])

    def shards(queries, keys, values, bucket_lens, gate, out_weight):
        rows_here, width = queries.shape[1:]
        share = width // outer
        length = bucket_lens[0]
        here = lax.axis_index("seq")
        row, own = here // inner, here % inner
        position = here * rows_here + lax.iota(jnp.int32, rows_here)
        pairs = cut_pieces(row[None], [keys[0], values[0]], outer)
        query = cut_pieces(row[None], [queries[0]], outer)
        pairs = [send(p, k) for k, p in enumerate(pairs)]
        query = [send(p, k) for k, p in enumerate(query)]
        groups = row ^ lax.iota(jnp.int32, outer)
        if inner == 2:
            pairs = pairs + [
                lax.ppermute(p, "seq", [(s, s ^ 1) for s in range(parts)]) for p in pairs
            ]
            members = jnp.stack([own, 1 - own])
        else:
            pairs = [
                lax.all_gather(
                    jnp.concatenate(pairs, axis=0), "seq", axis=0, tiled=True,
                    axis_index_groups=same_outer,
                )
            ]
            members = lax.iota(jnp.int32, inner)
        places = (
            (groups[None, :, None] * inner + members[:, None, None]) * rows_here
            + lax.iota(jnp.int32, rows_here)[None, None, :]
        )
        usable = (places < length).astype(jnp.int32).reshape(1, -1)
        outs = attend_pieces(usable, query, pairs)
        back = [send(p, k) for k, p in enumerate(outs)]
        weight = jnp.concatenate(
            [lax.dynamic_slice_in_dim(out_weight, (row ^ k) * share, share, 0) for k in range(outer)], axis=0
        )
        attended = jnp.concatenate(back, axis=1)
        everyone = lax.all_gather(attended, "bucket", axis=0, tiled=True)
        projected = jnp.dot(everyone, weight, preferred_element_type=jnp.float32)
        projected = projected.astype(jnp.bfloat16).reshape(-1, rows_here, out_weight.shape[1])
        gathered = lax.all_to_all(projected, "bucket", split_axis=0, concat_axis=0, tiled=True)
        wide_rows = jnp.concatenate([gathered[c] for c in range(gathered.shape[0])], axis=1)
        result = wide_rows.astype(jnp.float32) * gate[0][None, :]
        return jnp.where((position < length)[:, None], result, 0.0).astype(jnp.bfloat16)[None]

    return shards


def solution(mesh):
    placed = (
        P("bucket", "seq", None),
        P("bucket", "seq", None),
        P("bucket", "seq", None),
        P("bucket"),
        P("bucket", None),
        P(None, "bucket"),
    )
    return jax.shard_map(
        make_shards(mesh.shape["seq"]),
        mesh=mesh, in_specs=placed, out_specs=P("bucket", "seq", None), check_vma=False,
    )
```
